32 devices in a mesh: dp: 8 (over z, y), mp: 4 (over x, core).
Axes of the slice: x: 2, y: 2, z: 4, core: 2. Of those that a mesh axis runs over, the one named last changes fastest.
Arguments:
- pred_input: bfloat16 [512, 256, 384], P('dp'), may hold values from -6 to 6
- proj_weight: bfloat16 [384, 1280], P('dp', 'mp'), may hold values from -0.3125 to 0.3125
- proj_bias: float32 [1280], P('mp'), may hold values from -3 to 3
- targets: bfloat16 [512, 256, 1280], P('dp', None, 'mp'), may hold values from -6 to 6
- block_masks: int32 [512, 4, 256], P('dp'), may hold values from 0 to 1, as said below
Outputs:
- loss: float32 [], replicated
- clip_scale: float32 [], replicated
- grad_weight: float32 [384, 1280], P('dp', 'mp')
- grad_bias: float32 [1280], P('mp')
The draws below stay inside these ranges and needn't reach their ends.
Inputs may be any that keep to these rules, and one draw needn't show every extreme that they name: `block_masks`: each of an image's 4 target blocks is a nonempty rectangle of patches on the 16 x 16 grid (row-major patch order); blocks may intersect.
All inputs are finite; a program needn't handle non-finite values.
Results may differ from the reference program's by a relative error of at most 0.0003.
Values may be sent and summed in bfloat16 or wider, within the bound.
No kernel may reach another device: no remote copies, remote signals or barrier semaphores. Data moves between devices by JAX's collectives and lax.ppermute only.
A program may use at most 192 MiB of HBM per device.

```python
import jax
import jax.numpy as jnp
from jax import lax

D = 1280
E = 384
GRID = 16
BLOCKS = 4
IMG_DEV = 64
PATCHES = 256
IMAGES = 512


def draw_block_masks(key, part):
    keys = jax.random.split(key, 4)
    lowest = max(1, GRID * 5 // 16)
    highest = GRID // 2 + 1
    heights = jax.random.randint(keys[0], (IMAGES, BLOCKS, 1), lowest, highest)
    widths = jax.random.randint(keys[1], (IMAGES, BLOCKS, 1), lowest, highest)
    top_raw = jax.random.randint(keys[2], (IMAGES, BLOCKS, 1), 0, 1 << 20)
    left_raw = jax.random.randint(keys[3], (IMAGES, BLOCKS, 1), 0, 1 << 20)
    top_row = top_raw % (GRID - heights + 1)
    left_col = left_raw % (GRID - widths + 1)
    places = jnp.arange(GRID * GRID, dtype=jnp.int32)
    row_of = (places // GRID)[None, None, :]
    col_of = (places % GRID)[None, None, :]
    inside = (row_of >= top_row) & (row_of < top_row + heights) & (col_of >= left_col) & (col_of < left_col + widths)
    return inside.astype(jnp.int32)


def shard_levels(own_key, dims, pieces, low, high):
    level = 1.0
    for axis_at, blocks in pieces:
        draws = jax.random.uniform(jax.random.fold_in(jax.random.fold_in(own_key, 6), axis_at), (blocks,), jnp.float32, low / len(pieces), high / len(pieces))
        level = level * jnp.repeat(jnp.exp(draws), dims[axis_at] // blocks).reshape((-1,) + (1,) * (len(dims) - 1 - axis_at))
    return level


def scatter_about(rng, shape, spread, bound, pieces=(), held_as=jnp.bfloat16):
    values = spread * jax.random.normal(rng, shape, jnp.float32)
    if pieces:
        values = values * shard_levels(rng, shape, pieces, -0.22, 0.18)
    return jnp.clip(values, -bound, bound).astype(held_as)


def setup_inputs(seed: int = 0) -> dict:
    key_list = jax.random.split(jax.random.key(seed), 6)
    return {
        "pred_input": scatter_about(key_list[0], (IMAGES, PATCHES, E), 1.0, 6.0, ((0, 8),)),
        "proj_weight": scatter_about(key_list[1], (E, D), E ** -0.5, 0.3125, ((0, 8), (1, 4))),
        "proj_bias": scatter_about(key_list[2], (D,), 0.5, 3.0, ((0, 4),), jnp.float32),
        "targets": scatter_about(key_list[3], (IMAGES, PATCHES, D), 1.0, 6.0, ((0, 8), (2, 4))),
        "block_masks": draw_block_masks(jax.random.fold_in(key_list[5], 71), 0),
    }


def reference(pred_input, proj_weight, proj_bias, targets, block_masks):
    groups = IMAGES // IMG_DEV
    inputs_grouped = pred_input.reshape(groups, IMG_DEV * PATCHES, E)
    targets_grouped = targets.reshape(groups, IMG_DEV * PATCHES, D)
    coverage_all = lax.optimization_barrier(jnp.sum(block_masks, axis=1)).astype(jnp.float32)
    coverage_grouped = coverage_all.reshape(groups, IMG_DEV * PATCHES, 1)

    def step(carry, batch):
        grad_acc, bias_acc, loss_acc, count_acc = carry
        inputs_here, targets_here, coverage = batch
        target_f = targets_here.astype(jnp.float32)
        mean_feat = lax.optimization_barrier(jnp.mean(target_f, axis=1, keepdims=True))
        centered = target_f - mean_feat
        variance = lax.optimization_barrier(jnp.mean(centered * centered, axis=1, keepdims=True))
        tnorm = centered / jnp.sqrt(variance + 1e-05)
        pred = jnp.dot(inputs_here, proj_weight, preferred_element_type=jnp.float32) + proj_bias
        differ = pred - tnorm
        magnitude = jnp.abs(differ)
        smooth = jnp.where(magnitude < 1.0, 0.5 * differ * differ, magnitude - 0.5)
        clipped = coverage * jnp.clip(differ, -1.0, 1.0)
        source = clipped.astype(jnp.bfloat16)
        grad_acc = grad_acc + lax.dot_general(inputs_here, source, (((0,), (0,)), ((), ())), preferred_element_type=jnp.float32)
        bias_acc = bias_acc + lax.optimization_barrier(jnp.sum(clipped, axis=0))
        loss_acc = loss_acc + jnp.sum(coverage * smooth)
        count_acc = count_acc + jnp.sum(coverage)
        return ((grad_acc, bias_acc, loss_acc, count_acc), None)
    start = (jnp.zeros((E, D), jnp.float32), jnp.zeros((D,), jnp.float32), jnp.zeros((), jnp.float32), jnp.zeros((), jnp.float32))
    (grad_acc, bias_acc, loss_acc, total), unused = lax.scan(step, start, (inputs_grouped, targets_grouped, coverage_grouped))
    grad_w = grad_acc / total
    grad_b = bias_acc / total
    norm = jnp.sqrt(jnp.sum(grad_w * grad_w) + jnp.sum(grad_b * grad_b))
    clip_scale = jnp.minimum(1.0, 1.0 / (norm + 1e-06))
    loss = loss_acc / total / D
    return (loss, clip_scale, clip_scale * grad_w, clip_scale * grad_b)
```

```python
import functools

import jax
import jax.numpy as jnp
from jax import lax
from jax.experimental import pallas as pl
from jax.experimental.pallas import tpu as pltpu
from jax.sharding import PartitionSpec as P


F32, BF16 = jnp.float32, jnp.bfloat16
LANES = 128
STRIP = 16
EXTRA = 8


def divisor(count, most):
    return max(d for d in range(1, most + 1) if count % d == 0)


def stats_kernel(t_hbm, m_hbm, s_ref, cov_ref, t_buf, m_buf, t_sem, m_sem):
    images, feats, patches = t_buf.shape
    chunks = t_sem.shape[0]
    size = images // chunks

    def fetch(k):
        rows = pl.ds(k * size, size)
        return pltpu.make_async_copy(t_hbm.at[rows], t_buf.at[rows], t_sem.at[k])

    masks = pltpu.make_async_copy(m_hbm, m_buf, m_sem)
    for k in range(chunks):
        fetch(k).start()
    masks.start()
    masks.wait()

    def step(k, carry):
        fetch(k).wait()
        for j in range(size):
            image = k * size + j
            total = jnp.zeros((8, patches), F32)
            square = jnp.zeros((8, patches), F32)
            for r in range(0, feats, STRIP):
                t = t_buf[image, r : r + STRIP, :].astype(F32)
                for q in range(0, STRIP, 8):
                    u = t[q : q + 8]
                    total += u
                    square += u * u
            s_ref[0, pl.ds(image, 1), :] = jnp.sum(total, axis=0, keepdims=True)
            s_ref[1, pl.ds(image, 1), :] = jnp.sum(square, axis=0, keepdims=True)
            cov_ref[pl.ds(image, 1), :] = jnp.sum(m_buf[image], axis=0, keepdims=True).astype(F32)
        return carry

    lax.fori_loop(0, chunks, step, 0)


def patch_stats(targets, masks):
    images, feats, patches = targets.shape
    chunks = divisor(images, 16)
    return pl.pallas_call(
        stats_kernel,
        in_specs=[pl.BlockSpec(memory_space=pl.ANY)] * 2,
        out_specs=[pl.BlockSpec(memory_space=pltpu.VMEM)] * 2,
        out_shape=[
            jax.ShapeDtypeStruct((2, images, patches), F32),
            jax.ShapeDtypeStruct((images, patches), F32),
        ],
        scratch_shapes=[
            pltpu.VMEM(targets.shape, targets.dtype),
            pltpu.VMEM(masks.shape, masks.dtype),
            pltpu.SemaphoreType.DMA((chunks,)),
            pltpu.SemaphoreType.DMA,
        ],
        cost_estimate=pl.CostEstimate(
            flops=5_000_000_000, bytes_accessed=targets.size * 2, transcendentals=0
        ),
        name="patch_stats",
    )(targets, masks)


def loss_kernel(
    feats_full, dp_axis,
    s1_ref, s2_ref, cov_ref, w_ref, b_ref, t_hbm, x_hbm,
    keep_ref, send_ref,
    t_buf, x_buf, wt, bcol, rstd_s, shift_s, p0, p1, c0, c1, acc, bacc, lacc, t_sem, x_sem,
):
    images, feats, patches = t_buf.shape
    width = x_buf.shape[2]
    steps = t_sem.shape[0]
    size = images // steps
    group = size // 2
    halves = (p0, p1), (c0, c1)

    def fetch_t(k):
        rows = pl.ds(k * size, size)
        return pltpu.make_async_copy(t_hbm.at[rows], t_buf.at[rows], t_sem.at[k])

    def fetch_x(k):
        rows = pl.ds(k * size, size)
        return pltpu.make_async_copy(x_hbm.at[rows], x_buf.at[rows], x_sem.at[k])

    for k in range(steps):
        fetch_x(k).start()
        fetch_t(k).start()

    wt[...] = w_ref[...].T
    bcol[...] = jnp.broadcast_to(b_ref[...], (LANES, feats)).T
    acc[...] = jnp.zeros_like(acc)
    bacc[...] = jnp.zeros_like(bacc)
    lacc[...] = jnp.zeros_like(lacc)
    c1[...] = jnp.zeros_like(c1)
    mean = (s1_ref[0] + s2_ref[0]) * (1.0 / feats_full)
    var = (s1_ref[1] + s2_ref[1]) * (1.0 / feats_full) - mean * mean
    rstd = lax.rsqrt(var + 1e-05)
    rstd_s[...] = rstd
    shift_s[...] = mean * rstd

    def predict(slot, first):
        for j in range(group):
            halves[0][slot][j] = lax.dot_general(
                wt[...], x_buf[first + j], (((1,), (1,)), ((), ())), preferred_element_type=F32
            )

    def elementwise(slot, first):
        for j in range(group):
            image = first + j
            row = pl.ds(image, 1)
            rstd_row, shift_row, cover = rstd_s[row, :], shift_s[row, :], cov_ref[row, :]
            losses = jnp.zeros((8, patches), F32)
            for r in range(0, feats, STRIP):
                t = t_buf[image, r : r + STRIP, :].astype(F32)
                bias = jnp.concatenate([bcol[r : r + STRIP, :]] * (patches // LANES), axis=1)
                d = (halves[0][slot][j, r : r + STRIP, :] + bias) + (shift_row - t * rstd_row)
                c = jnp.minimum(jnp.maximum(d, -1.0), 1.0)
                h = c * (d - 0.5 * c)
                for q in range(0, STRIP, 8):
                    losses += h[q : q + 8]
                clipped = c * cover
                halves[1][slot][r : r + STRIP, j * patches : (j + 1) * patches] = clipped.astype(BF16)
                folded = clipped[:, :LANES]
                for q in range(LANES, patches, LANES):
                    folded += clipped[:, q : q + LANES]
                bacc[r : r + STRIP, :] += folded
            lacc[...] += losses * cover

    def accumulate(slot, first):
        rows = x_buf[pl.ds(first, group)].reshape(group * patches, width)
        acc[...] += jnp.dot(halves[1][slot][...], rows, preferred_element_type=F32)

    fetch_x(0).wait()
    predict(0, 0)

    def step(k, carry):
        base = k * size
        fetch_t(k).wait()

        @pl.when(k + 1 < steps)
        def _():
            fetch_x(k + 1).wait()

        predict(1, base + group)
        elementwise(0, base)
        accumulate(1, jnp.maximum(base - group, 0))
        predict(0, jnp.minimum(base + size, images - group))
        elementwise(1, base + group)
        accumulate(0, base)
        return carry

    lax.fori_loop(0, steps, step, 0)
    accumulate(1, images - group)

    grads = acc[...].T
    bias_row = jnp.sum(bacc[...].T, axis=0, keepdims=True)
    loss = jnp.sum(lacc[...])
    count = jnp.sum(cov_ref[...])
    lane = lax.broadcasted_iota(jnp.int32, (1, feats), 1)
    scalars = jnp.where(lane == 0, loss, jnp.where(lane == 1, count, 0.0))
    parts = lax.axis_size(dp_axis)
    rows = width // parts
    mine = lax.rem(lax.axis_index(dp_axis), 2)
    kept = keep_ref.shape[0] - EXTRA
    for ref in (keep_ref, send_ref):
        ref[kept : kept + 1, :] = bias_row
        ref[kept + 1 : kept + 2, :] = scalars
        ref[kept + 2 :, :] = jnp.zeros((EXTRA - 2, feats), F32)
    for bit in range(2):
        @pl.when(mine == bit)
        def _():
            for c in range(parts):
                ref = keep_ref if c % 2 == bit else send_ref
                at = (c // 2) * rows
                ref[at : at + rows, :] = grads[c * rows : (c + 1) * rows]


def loss_and_grads(s1, s2, cover, weight, bias, targets, inputs, feats_full, dp_axis):
    images, feats, patches = targets.shape
    width = inputs.shape[2]
    steps = divisor(images // 2, 16)
    size = images // steps
    if size % 2:
        steps, size = steps // 2, size * 2
    group = size // 2
    out = jax.ShapeDtypeStruct((width // 2 + EXTRA, feats), F32)
    return pl.pallas_call(
        functools.partial(loss_kernel, feats_full, dp_axis),
        in_specs=[pl.BlockSpec(memory_space=pltpu.VMEM)] * 5 + [pl.BlockSpec(memory_space=pl.ANY)] * 2,
        out_specs=[pl.BlockSpec(memory_space=pltpu.VMEM)] * 2,
        out_shape=[out, out],
        scratch_shapes=[
            pltpu.VMEM(targets.shape, targets.dtype),
            pltpu.VMEM(inputs.shape, inputs.dtype),
            pltpu.VMEM((feats, width), BF16),
            pltpu.VMEM((feats, LANES), F32),
            pltpu.VMEM((images, patches), F32),
            pltpu.VMEM((images, patches), F32),
            pltpu.VMEM((group, feats, patches), F32),
            pltpu.VMEM((group, feats, patches), F32),
            pltpu.VMEM((feats, group * patches), BF16),
            pltpu.VMEM((feats, group * patches), BF16),
            pltpu.VMEM((feats, width), F32),
            pltpu.VMEM((feats, LANES), F32),
            pltpu.VMEM((8, patches), F32),
            pltpu.SemaphoreType.DMA((steps,)),
            pltpu.SemaphoreType.DMA((steps,)),
        ],
        cost_estimate=pl.CostEstimate(
            flops=images * patches * feats * width * 4,
            bytes_accessed=(targets.size + inputs.size) * 2,
            transcendentals=0,
        ),
        name="loss_and_grads",
    )(s1, s2, cover, weight, bias, targets, inputs)


def square_kernel(dp_axis, keep_ref, recv_ref, g_ref, tail_ref, out_ref):
    rows = g_ref.shape[0]
    grads = keep_ref[:rows] + recv_ref[:rows]
    tail = keep_ref[rows:] + recv_ref[rows:]
    g_ref[...] = grads
    tail_ref[...] = tail
    first = lax.axis_index(dp_axis) == 0
    bias_square = jnp.sum(tail[0:1] * tail[0:1])
    loss = tail[1:2, 0:1]
    square = jnp.sum(grads * grads) + jnp.where(first, bias_square, 0.0)
    lane = lax.broadcasted_iota(jnp.int32, (1, LANES), 1)
    row = jnp.where(lane == 0, square, jnp.where((lane == 1) & first, loss, 0.0))
    out_ref[...] = jnp.broadcast_to(row, out_ref.shape)


def finish_kernel(feats_full, g_ref, tail_ref, all_ref, loss_ref, clip_ref, gw_ref, gb_ref):
    sums = jnp.sum(all_ref[...], axis=0, keepdims=True)
    square, loss = sums[:, 0:1], sums[:, 1:2]
    total = tail_ref[1:2, 1:2]
    norm = jnp.sqrt(square) / total
    clip = jnp.minimum(1.0, 1.0 / (norm + 1e-06))
    factor = clip / total
    loss_ref[...] = loss / total / feats_full
    clip_ref[...] = clip
    gw_ref[...] = g_ref[...] * factor
    gb_ref[...] = tail_ref[0:1] * factor


def pairs(size, bit):
    return [(i, i ^ bit) for i in range(size)]


def swap(value, axis, bit):
    return lax.ppermute(value, axis, pairs(lax.axis_size(axis), bit))


def bits_of(size):
    return [1 << b for b in range(size.bit_length() - 1)]


def gather_rows(weight, axis):
    size = lax.axis_size(axis)
    me = lax.axis_index(axis)
    rows, feats = weight.shape
    held = weight[None]
    for bit in reversed(bits_of(size)):
        other = swap(held, axis, bit)
        low = (me & bit) == 0
        first, second = jnp.where(low, held, other), jnp.where(low, other, held)
        held = jnp.stack([first, second], axis=1).reshape(-1, rows, feats)
    return held.reshape(size * rows, feats)


def body(pred_input, proj_weight, proj_bias, targets, block_masks):
    feats = targets.shape[2]
    feats_full = float(feats * lax.axis_size("mp"))
    turned = jnp.swapaxes(targets, 1, 2)
    weight = gather_rows(proj_weight, "dp")
    stats, cover = patch_stats(turned, block_masks)
    mp_bits = bits_of(lax.axis_size("mp"))
    for bit in mp_bits[:-1]:
        stats = stats + swap(stats, "mp", bit)
    other = swap(stats, "mp", mp_bits[-1])
    keep, send = loss_and_grads(
        stats, other, cover, weight, proj_bias[None], turned, pred_input, feats_full, "dp"
    )
    size = lax.axis_size("dp")
    me = lax.axis_index("dp")
    rows = pred_input.shape[2] // size
    dp_bits = bits_of(size)
    received = swap(send, "dp", dp_bits[0])
    parts = size // 2
    for bit in dp_bits[1:]:
        both = keep + received
        main = both[: parts * rows].reshape(parts // 2, 2, rows, feats)
        extra = both[parts * rows :]
        low = (me & bit) == 0
        mine = jnp.where(low, main[:, 0], main[:, 1]).reshape(-1, feats)
        theirs = jnp.where(low, main[:, 1], main[:, 0]).reshape(-1, feats)
        keep = jnp.concatenate([mine, extra], axis=0)
        received = swap(jnp.concatenate([theirs, extra], axis=0), "dp", bit)
        parts //= 2
    devices = size * lax.axis_size("mp")
    grads, tail, row = pl.pallas_call(
        functools.partial(square_kernel, "dp"),
        out_shape=[
            jax.ShapeDtypeStruct((rows, feats), F32),
            jax.ShapeDtypeStruct((EXTRA, feats), F32),
            jax.ShapeDtypeStruct((devices, LANES), F32),
        ],
        name="square",
    )(keep, received)
    every = lax.all_to_all(row, ("dp", "mp"), 0, 0, tiled=True)
    loss, clip, grad_weight, grad_bias = pl.pallas_call(
        functools.partial(finish_kernel, feats_full),
        out_shape=[
            jax.ShapeDtypeStruct((1, 1), F32),
            jax.ShapeDtypeStruct((1, 1), F32),
            jax.ShapeDtypeStruct((rows, feats), F32),
            jax.ShapeDtypeStruct((1, feats), F32),
        ],
        name="finish",
    )(grads, tail, every)
    return loss[0, 0], clip[0, 0], grad_weight, grad_bias[0]


def solution(mesh):
    in_specs = (
        P("dp", None, None),
        P("dp", "mp"),
        P("mp"),
        P("dp", None, "mp"),
        P("dp", None, None),
    )
    out_specs = (P(), P(), P("dp", "mp"), P("mp"))
    return jax.shard_map(body, mesh=mesh, in_specs=in_specs, out_specs=out_specs, check_vma=False)
```

```python
import functools
import math

import jax
import jax.numpy as jnp
from jax import lax
from jax.experimental import pallas as pl
from jax.experimental.pallas import tpu as pltpu
from jax.sharding import PartitionSpec as P


F32, BF16 = jnp.float32, jnp.bfloat16
LANES = 128
STRIP = 16
EXTRA = 8
DEPTH = 4
MIB = 1 << 20


def divisor(count, most):
    return max(d for d in range(1, most + 1) if count % d == 0)


def in_hbm(value):
    return pltpu.with_memory_space_constraint(value, pltpu.HBM)


def in_vmem(value):
    return pltpu.with_memory_space_constraint(value, pltpu.VMEM)


def pieces(rows, feats):
    whole, left = divmod(feats, LANES)
    out = [(0, rows, k * rows, (k * LANES, (k + 1) * LANES, 0)) for k in range(whole)]
    if left:
        share = LANES // left if LANES % left == 0 and rows % (LANES // left) == 0 else 1
        each = rows // share
        for k in range(share):
            out.append((k * each, (k + 1) * each, whole * rows, (whole * LANES, feats, k * left)))
    return out


def packed_rows(rows, feats):
    return max(where + hi - lo for lo, hi, where, _ in pieces(rows, feats))


def stats_kernel(t_hbm, m_hbm, s_ref, cov_ref, t_buf, m_buf, t_sem, m_sem):
    images, feats, patches = t_buf.shape
    chunks = t_sem.shape[0]
    size = images // chunks

    def fetch(k):
        rows = pl.ds(k * size, size)
        return pltpu.make_async_copy(t_hbm.at[rows], t_buf.at[rows], t_sem.at[k])

    masks = pltpu.make_async_copy(m_hbm, m_buf, m_sem)
    masks.start()
    for k in range(min(DEPTH, chunks)):
        fetch(k).start()
    masks.wait()

    def step(k, carry):
        @pl.when(k + DEPTH < chunks)
        def _():
            fetch(k + DEPTH).start()

        fetch(k).wait()
        for j in range(size):
            image = k * size + j
            total = jnp.zeros((8, patches), F32)
            square = jnp.zeros((8, patches), F32)
            for r in range(0, feats, STRIP):
                t = t_buf[image, r : r + STRIP, :].astype(F32)
                for q in range(0, STRIP, 8):
                    u = t[q : q + 8]
                    total += u
                    square += u * u
            s_ref[0, pl.ds(image, 1), :] = jnp.sum(total, axis=0, keepdims=True)
            s_ref[1, pl.ds(image, 1), :] = jnp.sum(square, axis=0, keepdims=True)
            cov_ref[pl.ds(image, 1), :] = jnp.sum(m_buf[image], axis=0, keepdims=True).astype(F32)
        return carry

    lax.fori_loop(0, chunks, step, 0)


def patch_stats(targets, masks):
    images, feats, patches = targets.shape
    chunks = divisor(images, 16)
    return pl.pallas_call(
        stats_kernel,
        in_specs=[pl.BlockSpec(memory_space=pltpu.HBM)] * 2,
        out_specs=[pl.BlockSpec(memory_space=pltpu.VMEM)] * 3,
        out_shape=[
            jax.ShapeDtypeStruct((2, images, patches), F32),
            jax.ShapeDtypeStruct((images, patches), F32),
            pltpu.VMEM(targets.shape, targets.dtype),
        ],
        scratch_shapes=[
            pltpu.VMEM(masks.shape, masks.dtype),
            pltpu.SemaphoreType.DMA((chunks,)),
            pltpu.SemaphoreType.DMA,
        ],
        cost_estimate=pl.CostEstimate(
            flops=5_000_000_000, bytes_accessed=targets.size * 2, transcendentals=0
        ),
        compiler_params=pltpu.CompilerParams(vmem_limit_bytes=20 * MIB),
        name="patch_stats",
    )(in_hbm(targets), in_hbm(masks))


def stage_kernel(x_hbm, x_ref, sem):
    copy = pltpu.make_async_copy(x_hbm.at[: x_ref.shape[0]], x_ref, sem)
    copy.start()
    copy.wait()


def stage_inputs(inputs, images):
    shape = (images,) + inputs.shape[1:]
    return pl.pallas_call(
        stage_kernel,
        in_specs=[pl.BlockSpec(memory_space=pltpu.HBM)],
        out_specs=pl.BlockSpec(memory_space=pltpu.VMEM),
        out_shape=pltpu.VMEM(shape, inputs.dtype),
        scratch_shapes=[pltpu.SemaphoreType.DMA],
        compiler_params=pltpu.CompilerParams(vmem_limit_bytes=20 * MIB),
        cost_estimate=pl.CostEstimate(
            flops=2_000_000_000, bytes_accessed=2 * inputs.size, transcendentals=0
        ),
        name="stage_inputs",
    )(in_hbm(inputs))


def loss_kernel(
    feats_full, dp_axis,
    s1_ref, s2_ref, cov_ref, w_ref, b_ref, t_ref, head_ref, x_hbm,
    keep_ref, send_ref,
    tail_ref, wt, bcol, rstd_s, shift_s, p0, p1, clip_s, acc, bacc, lacc, x_sem,
):
    images, feats, patches = t_ref.shape
    width = tail_ref.shape[2]
    head = head_ref.shape[0]
    steps = x_sem.shape[0]
    size = (images - head) // steps
    pred_s = p0, p1
    group = clip_s.shape[1] // patches

    def fetch(k):
        return pltpu.make_async_copy(
            x_hbm.at[pl.ds(head + k * size, size)], tail_ref.at[pl.ds(k * size, size)], x_sem.at[k]
        )

    for k in range(steps):
        fetch(k).start()

    wt[...] = w_ref[...].T
    bcol[...] = jnp.broadcast_to(b_ref[...].reshape(1, feats), (LANES, feats)).T
    acc[...] = jnp.zeros_like(acc)
    bacc[...] = jnp.zeros_like(bacc)
    lacc[...] = jnp.zeros_like(lacc)
    mean = (s1_ref[0] + s2_ref[0]) * (1.0 / feats_full)
    var = (s1_ref[1] + s2_ref[1]) * (1.0 / feats_full) - mean * mean
    rstd = lax.rsqrt(var + 1e-05)
    rstd_s[...] = rstd
    shift_s[...] = mean * rstd

    def predict(slot, x):
        pred_s[slot][...] = lax.dot_general(
            wt[...], x, (((1,), (1,)), ((), ())), preferred_element_type=F32
        )

    def elementwise(slot, image, at):
        row = pl.ds(image, 1)
        rstd_row, shift_row, cover = rstd_s[row, :], shift_s[row, :], cov_ref[row, :]
        losses = jnp.zeros((8, patches), F32)
        for r in range(0, feats, STRIP):
            t = t_ref[image, r : r + STRIP, :].astype(F32)
            bias = jnp.concatenate([bcol[r : r + STRIP, :]] * (patches // LANES), axis=1)
            d = (pred_s[slot][r : r + STRIP, :] + bias) + (shift_row - t * rstd_row)
            c = jnp.minimum(jnp.maximum(d, -1.0), 1.0)
            h = c * (d - 0.5 * c)
            for q in range(0, STRIP, 8):
                losses += h[q : q + 8]
            clipped = c * cover
            clip_s[r : r + STRIP, at * patches : (at + 1) * patches] = clipped.astype(BF16)
            folded = clipped[:, :LANES]
            for q in range(LANES, patches, LANES):
                folded += clipped[:, q : q + LANES]
            bacc[r : r + STRIP, :] += folded
        lacc[...] += losses * cover

    def run(x_ref, first, base, count):
        predict(0, x_ref[base])
        for g in range(count):
            if g + 1 < count:
                predict((g + 1) % 2, x_ref[base + g + 1])
            elementwise(g % 2, first + base + g, g % group)
            if (g + 1) % group == 0:
                rows = x_ref[pl.ds(base + g + 1 - group, group)].reshape(group * patches, width)
                acc[...] += jnp.dot(clip_s[...], rows, preferred_element_type=F32)

    def head_step(k, carry):
        run(head_ref, 0, k * size, size)
        return carry

    def tail_step(k, carry):
        fetch(k).wait()
        run(tail_ref, head, k * size, size)
        return carry

    lax.fori_loop(0, head // size, head_step, 0)
    lax.fori_loop(0, steps, tail_step, 0)

    grads = acc[...].T
    bias_row = jnp.sum(bacc[...].T, axis=0, keepdims=True)
    loss = jnp.sum(lacc[...])
    count = jnp.sum(cov_ref[...])
    lane = lax.broadcasted_iota(jnp.int32, (1, LANES), 1)
    scalars = jnp.where(lane == 0, loss, jnp.where(lane == 1, count, 0.0))
    parts = lax.axis_size(dp_axis)
    rows = width // parts
    mine = lax.rem(lax.axis_index(dp_axis), 2)
    block = packed_rows(rows, feats)
    kept = (parts // 2) * block
    tail = jnp.zeros((EXTRA, LANES), F32)
    for ref in (keep_ref, send_ref):
        ref[kept:, :] = tail
        for k in range(-(-feats // LANES)):
            wide = min(LANES, feats - k * LANES)
            ref[kept + k : kept + k + 1, :wide] = bias_row[:, k * LANES : k * LANES + wide]
        ref[kept + EXTRA - 1 :, :] = scalars
    for bit in range(2):
        @pl.when(mine == bit)
        def _():
            for c in range(parts):
                ref = keep_ref if c % 2 == bit else send_ref
                at = (c // 2) * block
                for lo, hi, where, lanes in pieces(rows, feats):
                    ref[at + where : at + where + hi - lo, lanes[2] : lanes[2] + lanes[1] - lanes[0]] = grads[
                        c * rows + lo : c * rows + hi, lanes[0] : lanes[1]
                    ]


def loss_and_grads(s1, s2, cover, weight, bias, targets, head, inputs, feats_full, dp_axis):
    images, feats, patches = targets.shape
    width = inputs.shape[2]
    rest = images - head.shape[0]
    size = divisor(math.gcd(rest, head.shape[0]), 16)
    group = divisor(size, 2)
    parts = lax.axis_size(dp_axis)
    rows = (parts // 2) * packed_rows(width // parts, feats) + EXTRA
    out = jax.ShapeDtypeStruct((rows, LANES), F32)
    return pl.pallas_call(
        functools.partial(loss_kernel, feats_full, dp_axis),
        in_specs=[pl.BlockSpec(memory_space=pltpu.VMEM)] * 7 + [pl.BlockSpec(memory_space=pltpu.HBM)],
        out_specs=[pl.BlockSpec(memory_space=pltpu.VMEM)] * 2,
        out_shape=[out, out],
        scratch_shapes=[
            pltpu.VMEM((rest,) + inputs.shape[1:], inputs.dtype),
            pltpu.VMEM((feats, width), BF16),
            pltpu.VMEM((feats, LANES), F32),
            pltpu.VMEM((images, patches), F32),
            pltpu.VMEM((images, patches), F32),
            pltpu.VMEM((feats, patches), F32),
            pltpu.VMEM((feats, patches), F32),
            pltpu.VMEM((feats, group * patches), BF16),
            pltpu.VMEM((feats, width), F32),
            pltpu.VMEM((feats, LANES), F32),
            pltpu.VMEM((8, patches), F32),
            pltpu.SemaphoreType.DMA((rest // size,)),
        ],
        compiler_params=pltpu.CompilerParams(vmem_limit_bytes=36 * MIB),
        cost_estimate=pl.CostEstimate(
            flops=images * patches * feats * width * 4,
            bytes_accessed=(targets.size + inputs.size) * 2,
            transcendentals=0,
        ),
        name="loss_and_grads",
    )(s1, s2, cover, weight, bias, in_vmem(targets), in_vmem(head), in_hbm(inputs))


def square_kernel(dp_axis, keep_ref, recv_ref, g_ref, tail_ref, out_ref):
    rows, feats = g_ref.shape
    block = packed_rows(rows, feats)
    both = keep_ref[...] + recv_ref[...]
    for lo, hi, where, lanes in pieces(rows, feats):
        g_ref[lo:hi, lanes[0] : lanes[1]] = both[
            where : where + hi - lo, lanes[2] : lanes[2] + lanes[1] - lanes[0]
        ]
    tail_ref[...] = both[block:]
    first = lax.axis_index(dp_axis) == 0
    grads = g_ref[...]
    bias = both[block : block + EXTRA - 1]
    loss = both[block + EXTRA - 1 :, 0:1]
    square = jnp.sum(grads * grads) + jnp.where(first, jnp.sum(bias * bias), 0.0)
    lane = lax.broadcasted_iota(jnp.int32, (1, LANES), 1)
    row = jnp.where(lane == 0, square, jnp.where((lane == 1) & first, loss, 0.0))
    out_ref[...] = jnp.broadcast_to(row, out_ref.shape)


def finish_kernel(feats_full, g_ref, tail_ref, all_ref, loss_ref, clip_ref, gw_ref, gb_ref):
    sums = jnp.sum(all_ref[...], axis=0, keepdims=True)
    square, loss = sums[:, 0:1], sums[:, 1:2]
    total = tail_ref[EXTRA - 1 :, 1:2]
    norm = jnp.sqrt(square) / total
    clip = jnp.minimum(1.0, 1.0 / (norm + 1e-06))
    factor = clip / total
    loss_ref[...] = loss / total / feats_full
    clip_ref[...] = clip
    gw_ref[...] = g_ref[...] * factor
    feats = gb_ref.shape[0]
    bias = tail_ref[...] * factor
    row = jnp.concatenate([bias[k : k + 1] for k in range(-(-feats // LANES))], axis=1)
    gb_ref[...] = row[:, :feats].reshape(feats)


def pairs(size, bit):
    return [(i, i ^ bit) for i in range(size)]


def swap(value, axis, bit):
    return lax.ppermute(value, axis, pairs(lax.axis_size(axis), bit))


def bits_of(size):
    return [1 << b for b in range(size.bit_length() - 1)]


def gather_far(weight, axis):
    size = lax.axis_size(axis)
    return [weight] + [swap(weight, axis, far) for far in range(2, size, 2)]


def gather_near(parts, lows, axis):
    rows, feats = parts[0].shape
    half = len(parts)
    for bit in bits_of(half):
        low = lows[2 * bit]
        parts = [jnp.where(low, parts[j], parts[j ^ bit]) for j in range(half)]
    far = jnp.stack(parts)
    other = swap(far, axis, 1)
    low = lows[1]
    first, second = jnp.where(low, far, other), jnp.where(low, other, far)
    return jnp.stack([first, second], axis=1).reshape(2 * half * rows, feats)


def body(pred_input, proj_weight, proj_bias, targets, block_masks):
    feats = targets.shape[2]
    feats_full = float(feats * lax.axis_size("mp"))
    turned = jnp.swapaxes(targets, 1, 2)
    size = lax.axis_size("dp")
    me = lax.axis_index("dp")
    lows = {bit: (me & bit) == 0 for bit in bits_of(size)}
    lows, block_masks = lax.optimization_barrier((lows, block_masks))
    parts = gather_far(proj_weight, "dp")
    stats, cover, turned = patch_stats(turned, block_masks)
    parts, stats = lax.optimization_barrier((parts, stats))
    weight = gather_near(parts, lows, "dp")
    mp_bits = bits_of(lax.axis_size("mp"))
    for bit in mp_bits[:-1]:
        stats = stats + swap(stats, "mp", bit)
    other = swap(stats, "mp", mp_bits[-1])
    staged = stage_inputs(lax.optimization_barrier((pred_input, stats))[0], targets.shape[0] // 2)
    keep, send = loss_and_grads(
        stats, other, cover, weight, proj_bias, turned, staged, pred_input, feats_full, "dp"
    )
    rows = pred_input.shape[2] // size
    block = packed_rows(rows, feats)
    dp_bits = bits_of(size)
    received = swap(send, "dp", dp_bits[0])
    parts = size // 2
    for bit in dp_bits[1:]:
        both = keep + received
        main = both[: parts * block].reshape(parts // 2, 2, block, LANES)
        extra = both[parts * block :]
        low = lows[bit]
        mine = jnp.where(low, main[:, 0], main[:, 1]).reshape(-1, LANES)
        theirs = jnp.where(low, main[:, 1], main[:, 0]).reshape(-1, LANES)
        keep = jnp.concatenate([mine, extra], axis=0)
        received = swap(jnp.concatenate([theirs, extra], axis=0), "dp", bit)
        parts //= 2
    devices = size * lax.axis_size("mp")
    grads, tail, row = pl.pallas_call(
        functools.partial(square_kernel, "dp"),
        out_shape=[
            jax.ShapeDtypeStruct((rows, feats), F32),
            jax.ShapeDtypeStruct((EXTRA, LANES), F32),
            jax.ShapeDtypeStruct((devices, LANES), F32),
        ],
        compiler_params=pltpu.CompilerParams(vmem_limit_bytes=4 * MIB),
        name="square",
    )(keep, received)
    every = lax.all_to_all(row, ("dp", "mp"), 0, 0, tiled=True)
    loss, clip, grad_weight, grad_bias = pl.pallas_call(
        functools.partial(finish_kernel, feats_full),
        out_shape=[
            jax.ShapeDtypeStruct((1, 1), F32),
            jax.ShapeDtypeStruct((1, 1), F32),
            jax.ShapeDtypeStruct((rows, feats), F32),
            jax.ShapeDtypeStruct((feats,), F32),
        ],
        compiler_params=pltpu.CompilerParams(vmem_limit_bytes=4 * MIB),
        name="finish",
    )(grads, tail, every)
    return loss[0, 0], clip[0, 0], grad_weight, grad_bias


def solution(mesh):
    in_specs = (
        P("dp", None, None),
        P("dp", "mp"),
        P("mp"),
        P("dp", None, "mp"),
        P("dp", None, None),
    )
    out_specs = (P(), P(), P("dp", "mp"), P("mp"))
    return jax.shard_map(body, mesh=mesh, in_specs=in_specs, out_specs=out_specs, check_vma=False)
```

```python
import functools
import math

import jax
import jax.numpy as jnp
from jax import lax
from jax.experimental import pallas as pl
from jax.experimental.pallas import tpu as pltpu
from jax.sharding import PartitionSpec as P


F32, BF16 = jnp.float32, jnp.bfloat16
LANES = 128
STRIP = 16
EXTRA = 8
DEPTH = 8
MIB = 1 << 20


def divisor(count, most):
    return max(d for d in range(1, most + 1) if count % d == 0)


def in_hbm(value):
    return pltpu.with_memory_space_constraint(value, pltpu.HBM)


def in_vmem(value):
    return pltpu.with_memory_space_constraint(value, pltpu.VMEM)


def pieces(rows, feats):
    whole, left = divmod(feats, LANES)
    out = [(0, rows, k * rows, (k * LANES, (k + 1) * LANES, 0)) for k in range(whole)]
    if left:
        share = LANES // left if LANES % left == 0 and rows % (LANES // left) == 0 else 1
        each = rows // share
        for k in range(share):
            out.append((k * each, (k + 1) * each, whole * rows, (whole * LANES, feats, k * left)))
    return out


def packed_rows(rows, feats):
    return max(where + hi - lo for lo, hi, where, _ in pieces(rows, feats))


def cut_rows(rows, feats):
    return -(-packed_rows(rows, feats) // 16) * 8


def stats_kernel(t_hbm, s_ref, t_buf, t_sem):
    images, feats, patches = t_buf.shape
    chunks = t_sem.shape[0]
    size = images // chunks

    def fetch(k):
        rows = pl.ds(k * size, size)
        return pltpu.make_async_copy(t_hbm.at[rows], t_buf.at[rows], t_sem.at[k])

    for k in range(min(DEPTH, chunks)):
        fetch(k).start()

    def step(k, carry):
        @pl.when(k + DEPTH < chunks)
        def _():
            fetch(k + DEPTH).start()

        fetch(k).wait()
        for j in range(size):
            image = k * size + j
            total = jnp.zeros((8, patches), F32)
            square = jnp.zeros((8, patches), F32)
            for r in range(0, feats, STRIP):
                t = t_buf[image, r : r + STRIP, :].astype(F32)
                for q in range(0, STRIP, 8):
                    u = t[q : q + 8]
                    total += u
                    square += u * u
            s_ref[0, pl.ds(image, 1), :] = jnp.sum(total, axis=0, keepdims=True)
            s_ref[1, pl.ds(image, 1), :] = jnp.sum(square, axis=0, keepdims=True)
        return carry

    lax.fori_loop(0, chunks, step, 0)


def patch_stats(targets):
    images, feats, patches = targets.shape
    chunks = divisor(images, 16)
    return pl.pallas_call(
        stats_kernel,
        in_specs=[pl.BlockSpec(memory_space=pltpu.HBM)],
        out_specs=[pl.BlockSpec(memory_space=pltpu.VMEM)] * 2,
        out_shape=[
            jax.ShapeDtypeStruct((2, images, patches), F32),
            pltpu.VMEM(targets.shape, targets.dtype),
        ],
        scratch_shapes=[
            pltpu.SemaphoreType.DMA((chunks,)),
        ],
        cost_estimate=pl.CostEstimate(
            flops=5_000_000_000, bytes_accessed=targets.size * 2, transcendentals=0
        ),
        compiler_params=pltpu.CompilerParams(vmem_limit_bytes=20 * MIB),
        name="patch_stats",
    )(in_hbm(targets))


def stage_kernel(x_hbm, m_ref, x_ref, cov_ref, sem):
    copy = pltpu.make_async_copy(x_hbm.at[: x_ref.shape[0]], x_ref, sem)
    copy.start()
    for image in range(m_ref.shape[0]):
        cov_ref[image : image + 1, :] = jnp.sum(m_ref[image], axis=0, keepdims=True).astype(F32)
    copy.wait()


def stage_inputs(inputs, masks, images):
    shape = (images,) + inputs.shape[1:]
    return pl.pallas_call(
        stage_kernel,
        in_specs=[pl.BlockSpec(memory_space=pltpu.HBM), pl.BlockSpec(memory_space=pltpu.VMEM)],
        out_specs=[pl.BlockSpec(memory_space=pltpu.VMEM)] * 2,
        out_shape=[
            pltpu.VMEM(shape, inputs.dtype),
            jax.ShapeDtypeStruct((masks.shape[0], masks.shape[2]), F32),
        ],
        scratch_shapes=[pltpu.SemaphoreType.DMA],
        compiler_params=pltpu.CompilerParams(vmem_limit_bytes=20 * MIB),
        cost_estimate=pl.CostEstimate(
            flops=2_000_000_000, bytes_accessed=2 * inputs.size, transcendentals=0
        ),
        name="stage_inputs",
    )(in_hbm(inputs), masks)


def loss_kernel(
    feats_full, dp_axis,
    s1_ref, s2_ref, cov_ref, w_ref, b_ref, t_ref, head_ref, x_hbm,
    keep_a, send_a, keep_b, send_b,
    tail_ref, wt, bcol, rstd_s, shift_s, p0, p1, clip_s, acc, bacc, lacc, x_sem,
):
    images, feats, patches = t_ref.shape
    width = tail_ref.shape[2]
    head = head_ref.shape[0]
    steps = x_sem.shape[0]
    size = (images - head) // steps
    pred_s = p0, p1
    group = clip_s.shape[1] // patches

    def fetch(k):
        return pltpu.make_async_copy(
            x_hbm.at[pl.ds(head + k * size, size)], tail_ref.at[pl.ds(k * size, size)], x_sem.at[k]
        )

    for k in range(steps):
        fetch(k).start()

    wt[...] = w_ref[...].T
    bcol[...] = jnp.broadcast_to(b_ref[...].reshape(1, feats), (LANES, feats)).T
    acc[...] = jnp.zeros_like(acc)
    bacc[...] = jnp.zeros_like(bacc)
    lacc[...] = jnp.zeros_like(lacc)
    mean = (s1_ref[0] + s2_ref[0]) * (1.0 / feats_full)
    var = (s1_ref[1] + s2_ref[1]) * (1.0 / feats_full) - mean * mean
    rstd = lax.rsqrt(var + 1e-05)
    rstd_s[...] = rstd
    shift_s[...] = mean * rstd

    def predict(slot, x):
        pred_s[slot][...] = lax.dot_general(
            wt[...], x, (((1,), (1,)), ((), ())), preferred_element_type=F32
        )

    def elementwise(slot, image, at):
        row = pl.ds(image, 1)
        rstd_row, shift_row, cover = rstd_s[row, :], shift_s[row, :], cov_ref[row, :]
        losses = jnp.zeros((8, patches), F32)
        for r in range(0, feats, STRIP):
            t = t_ref[image, r : r + STRIP, :].astype(F32)
            bias = jnp.concatenate([bcol[r : r + STRIP, :]] * (patches // LANES), axis=1)
            d = (pred_s[slot][r : r + STRIP, :] + bias) + (shift_row - t * rstd_row)
            c = jnp.minimum(jnp.maximum(d, -1.0), 1.0)
            h = c * (d - 0.5 * c)
            for q in range(0, STRIP, 8):
                losses += h[q : q + 8]
            clipped = c * cover
            clip_s[r : r + STRIP, at * patches : (at + 1) * patches] = clipped.astype(BF16)
            folded = clipped[:, :LANES]
            for q in range(LANES, patches, LANES):
                folded += clipped[:, q : q + LANES]
            bacc[r : r + STRIP, :] += folded
        lacc[...] += losses * cover

    def run(x_ref, first, base, count):
        predict(0, x_ref[base])
        for g in range(count):
            if g + 1 < count:
                predict((g + 1) % 2, x_ref[base + g + 1])
            elementwise(g % 2, first + base + g, g % group)
            if (g + 1) % group == 0:
                rows = x_ref[pl.ds(base + g + 1 - group, group)].reshape(group * patches, width)
                acc[...] += jnp.dot(clip_s[...], rows, preferred_element_type=F32)

    def head_step(k, carry):
        run(head_ref, 0, k * size, size)
        return carry

    def tail_step(k, carry):
        fetch(k).wait()
        run(tail_ref, head, k * size, size)
        return carry

    lax.fori_loop(0, head // size, head_step, 0)
    lax.fori_loop(0, steps, tail_step, 0)

    grads = acc[...].T
    bias_row = jnp.sum(bacc[...].T, axis=0, keepdims=True)
    loss = jnp.sum(lacc[...])
    count = jnp.sum(cov_ref[...])
    lane = lax.broadcasted_iota(jnp.int32, (1, LANES), 1)
    scalars = jnp.where(lane == 0, loss, jnp.where(lane == 1, count, 0.0))
    parts = lax.axis_size(dp_axis)
    rows = width // parts
    me = lax.axis_index(dp_axis)
    cut, block = cut_rows(rows, feats), packed_rows(rows, feats)
    kept = (parts // 2) * cut
    for ref in (keep_a, send_a):
        ref[kept:, :] = jnp.zeros((EXTRA, LANES), F32)
        for k in range(-(-feats // LANES)):
            wide = min(LANES, feats - k * LANES)
            ref[kept + k : kept + k + 1, :wide] = bias_row[:, k * LANES : k * LANES + wide]
        ref[kept + EXTRA - 1 :, :] = scalars

    def put(ref, at, c, first, last):
        for lo, hi, where, (here, end, there) in pieces(rows, feats):
            low, high = max(where, first), min(where + hi - lo, last)
            if low < high:
                row = c * rows + lo + low - where
                ref[at + low - first : at + high - first, there : there + end - here] = grads[
                    row : row + high - low, here:end
                ]

    for bit in range(2):
        @pl.when(lax.rem(me, 2) == bit)
        def _():
            for c in range(parts):
                put(keep_a if c % 2 == bit else send_a, (c // 2) * cut, c, 0, cut)

        @pl.when(lax.rem(lax.div(me, 2), 2) == bit)
        def _():
            for c in range(parts):
                at = (c // 4 * 2 + c % 2) * (block - cut)
                put(keep_b if c // 2 % 2 == bit else send_b, at, c, cut, block)


def loss_and_grads(s1, s2, cover, weight, bias, targets, head, inputs, feats_full, dp_axis):
    images, feats, patches = targets.shape
    width = inputs.shape[2]
    rest = images - head.shape[0]
    size = divisor(math.gcd(rest, head.shape[0]), 16)
    group = divisor(size, 2)
    parts = lax.axis_size(dp_axis)
    cut, block = cut_rows(width // parts, feats), packed_rows(width // parts, feats)
    out_a = jax.ShapeDtypeStruct(((parts // 2) * cut + EXTRA, LANES), F32)
    out_b = jax.ShapeDtypeStruct(((parts // 2) * (block - cut), LANES), F32)
    return pl.pallas_call(
        functools.partial(loss_kernel, feats_full, dp_axis),
        in_specs=[pl.BlockSpec(memory_space=pltpu.VMEM)] * 7 + [pl.BlockSpec(memory_space=pltpu.HBM)],
        out_specs=[pl.BlockSpec(memory_space=pltpu.VMEM)] * 4,
        out_shape=[out_a, out_a, out_b, out_b],
        scratch_shapes=[
            pltpu.VMEM((rest,) + inputs.shape[1:], inputs.dtype),
            pltpu.VMEM((feats, width), BF16),
            pltpu.VMEM((feats, LANES), F32),
            pltpu.VMEM((images, patches), F32),
            pltpu.VMEM((images, patches), F32),
            pltpu.VMEM((feats, patches), F32),
            pltpu.VMEM((feats, patches), F32),
            pltpu.VMEM((feats, group * patches), BF16),
            pltpu.VMEM((feats, width), F32),
            pltpu.VMEM((feats, LANES), F32),
            pltpu.VMEM((8, patches), F32),
            pltpu.SemaphoreType.DMA((rest // size,)),
        ],
        compiler_params=pltpu.CompilerParams(vmem_limit_bytes=36 * MIB),
        cost_estimate=pl.CostEstimate(
            flops=images * patches * feats * width * 4,
            bytes_accessed=(targets.size + inputs.size) * 2,
            transcendentals=0,
        ),
        name="loss_and_grads",
    )(s1, s2, cover, weight, bias, in_vmem(targets), in_vmem(head), in_hbm(inputs))


def square_kernel(dp_axis, keep_ref, recv_ref, g_ref, tail_ref, out_ref):
    rows, feats = g_ref.shape
    block = packed_rows(rows, feats)
    both = keep_ref[...] + recv_ref[...]
    for lo, hi, where, lanes in pieces(rows, feats):
        g_ref[lo:hi, lanes[0] : lanes[1]] = both[
            where : where + hi - lo, lanes[2] : lanes[2] + lanes[1] - lanes[0]
        ]
    tail_ref[...] = both[block:]
    first = lax.axis_index(dp_axis) == 0
    grads = g_ref[...]
    bias = both[block : block + EXTRA - 1]
    loss = both[block + EXTRA - 1 :, 0:1]
    square = jnp.sum(grads * grads) + jnp.where(first, jnp.sum(bias * bias), 0.0)
    lane = lax.broadcasted_iota(jnp.int32, (1, LANES), 1)
    row = jnp.where(lane == 0, square, jnp.where((lane == 1) & first, loss, 0.0))
    out_ref[...] = jnp.broadcast_to(row, out_ref.shape)


def finish_kernel(feats_full, g_ref, tail_ref, all_ref, loss_ref, clip_ref, gw_ref, gb_ref):
    sums = jnp.sum(all_ref[...], axis=0, keepdims=True)
    square, loss = sums[:, 0:1], sums[:, 1:2]
    total = tail_ref[EXTRA - 1 :, 1:2]
    norm = jnp.sqrt(square) / total
    clip = jnp.minimum(1.0, 1.0 / (norm + 1e-06))
    factor = clip / total
    loss_ref[...] = loss / total / feats_full
    clip_ref[...] = clip
    gw_ref[...] = g_ref[...] * factor
    feats = gb_ref.shape[0]
    bias = tail_ref[...] * factor
    row = jnp.concatenate([bias[k : k + 1] for k in range(-(-feats // LANES))], axis=1)
    gb_ref[...] = row[:, :feats].reshape(feats)


def pairs(size, bit):
    return [(i, i ^ bit) for i in range(size)]


def swap(value, axis, bit):
    return lax.ppermute(value, axis, pairs(lax.axis_size(axis), bit))


def bits_of(size):
    return [1 << b for b in range(size.bit_length() - 1)]


def gather_far(weight, axis):
    size = lax.axis_size(axis)
    return [weight] + [swap(weight, axis, far) for far in range(2, size, 2)]


def swap_near(parts, lows, axis):
    half = len(parts)
    for bit in bits_of(half):
        low = lows[2 * bit]
        parts = [jnp.where(low, parts[j], parts[j ^ bit]) for j in range(half)]
    far = jnp.stack(parts)
    return far, swap(far, axis, 1)


def join_near(far, near, lows):
    half, rows, feats = far.shape
    low = lows[1]
    first, second = jnp.where(low, far, near), jnp.where(low, near, far)
    return jnp.stack([first, second], axis=1).reshape(2 * half * rows, feats)


def halve(value, block, low):
    pair = value.reshape(-1, 2, block, LANES)
    stay, go = jnp.where(low, pair[:, 0], pair[:, 1]), jnp.where(low, pair[:, 1], pair[:, 0])
    return stay.reshape(-1, LANES), go.reshape(-1, LANES)


def body(pred_input, proj_weight, proj_bias, targets, block_masks):
    feats = targets.shape[2]
    feats_full = float(feats * lax.axis_size("mp"))
    turned = jnp.swapaxes(targets, 1, 2)
    size = lax.axis_size("dp")
    me = lax.axis_index("dp")
    lows = {bit: (me & bit) == 0 for bit in bits_of(size)}
    lows, turned, proj_weight = lax.optimization_barrier((lows, turned, proj_weight))
    parts = gather_far(proj_weight, "dp")
    stats, turned = patch_stats(turned)
    parts, stats = lax.optimization_barrier((parts, stats))
    far, near = swap_near(parts, lows, "dp")
    mp_bits = bits_of(lax.axis_size("mp"))
    for bit in mp_bits[:-1]:
        stats = stats + swap(stats, "mp", bit)
    other = swap(stats, "mp", mp_bits[-1])
    staged, cover = stage_inputs(
        lax.optimization_barrier((pred_input, stats))[0], block_masks, targets.shape[0] // 2
    )
    near, staged = lax.optimization_barrier((near, staged))
    weight = join_near(far, near, lows)
    keep_a, send_a, keep_b, send_b = loss_and_grads(
        stats, other, cover, weight, proj_bias, turned, staged, pred_input, feats_full, "dp"
    )
    rows = pred_input.shape[2] // size
    cut, block = cut_rows(rows, feats), packed_rows(rows, feats)
    rest = block - cut
    parts = size // 2
    got_a, got_b = swap(send_a, "dp", 1), swap(send_b, "dp", 2)
    both_a = keep_a + got_a
    keep_a, send_a = halve(both_a[: parts * cut], cut, lows[2])
    extra = both_a[parts * cut :]
    got_a = swap(jnp.concatenate([send_a, extra], axis=0), "dp", 2)
    keep_b, send_b = halve(keep_b + got_b, rest, lows[1])
    got_b = swap(send_b, "dp", 1)
    parts //= 2
    both_a = jnp.concatenate([keep_a, extra], axis=0) + got_a
    extra = both_a[parts * cut :]
    main = jnp.concatenate(
        [both_a[: parts * cut].reshape(parts, cut, LANES), (keep_b + got_b).reshape(parts, rest, LANES)], axis=1
    ).reshape(parts * block, LANES)
    for bit in bits_of(size)[2:]:
        keep, send = halve(main, block, lows[bit])
        keep = jnp.concatenate([keep, extra], axis=0)
        received = swap(jnp.concatenate([send, extra], axis=0), "dp", bit)
        parts //= 2
        if parts > 1:
            both = keep + received
            main, extra = both[: parts * block], both[parts * block :]
    devices = size * lax.axis_size("mp")
    grads, tail, row = pl.pallas_call(
        functools.partial(square_kernel, "dp"),
        out_shape=[
            jax.ShapeDtypeStruct((rows, feats), F32),
            jax.ShapeDtypeStruct((EXTRA, LANES), F32),
            jax.ShapeDtypeStruct((devices, LANES), F32),
        ],
        compiler_params=pltpu.CompilerParams(vmem_limit_bytes=4 * MIB),
        name="square",
    )(keep, received)
    every = lax.all_to_all(row, ("dp", "mp"), 0, 0, tiled=True)
    loss, clip, grad_weight, grad_bias = pl.pallas_call(
        functools.partial(finish_kernel, feats_full),
        out_shape=[
            jax.ShapeDtypeStruct((1, 1), F32),
            jax.ShapeDtypeStruct((1, 1), F32),
            jax.ShapeDtypeStruct((rows, feats), F32),
            jax.ShapeDtypeStruct((feats,), F32),
        ],
        compiler_params=pltpu.CompilerParams(vmem_limit_bytes=4 * MIB),
        name="finish",
    )(grads, tail, every)
    return loss[0, 0], clip[0, 0], grad_weight, grad_bias


def solution(mesh):
    in_specs = (
        P("dp", None, None),
        P("dp", "mp"),
        P("mp"),
        P("dp", None, "mp"),
        P("dp", None, None),
    )
    out_specs = (P(), P(), P("dp", "mp"), P("mp"))
    return jax.shard_map(body, mesh=mesh, in_specs=in_specs, out_specs=out_specs, check_vma=False)
```

```python
import functools
import math

import jax
import jax.numpy as jnp
from jax import lax
from jax.experimental import pallas as pl
from jax.experimental.pallas import tpu as pltpu
from jax.sharding import PartitionSpec as P


F32, BF16 = jnp.float32, jnp.bfloat16
LANES = 128
STRIP = 16
EXTRA = 8
DEPTH = 8
MIB = 1 << 20


def divisor(count, most):
    return max(d for d in range(1, most + 1) if count % d == 0)


def in_hbm(value):
    return pltpu.with_memory_space_constraint(value, pltpu.HBM)


def in_vmem(value):
    return pltpu.with_memory_space_constraint(value, pltpu.VMEM)


def pieces(rows, feats):
    whole, left = divmod(feats, LANES)
    out = [(0, rows, k * rows, (k * LANES, (k + 1) * LANES, 0)) for k in range(whole)]
    if left:
        share = LANES // left if LANES % left == 0 and rows % (LANES // left) == 0 else 1
        each = rows // share
        for k in range(share):
            out.append((k * each, (k + 1) * each, whole * rows, (whole * LANES, feats, k * left)))
    return out


def packed_rows(rows, feats):
    return max(where + hi - lo for lo, hi, where, _ in pieces(rows, feats))


def cut_rows(rows, feats):
    return -(-packed_rows(rows, feats) // 16) * 8


def stats_kernel(t_hbm, s_ref, t_buf, t_sem):
    images, feats, patches = t_buf.shape
    chunks = t_sem.shape[0]
    size = images // chunks

    def fetch(k):
        rows = pl.ds(k * size, size)
        return pltpu.make_async_copy(t_hbm.at[rows], t_buf.at[rows], t_sem.at[k])

    for k in range(min(DEPTH, chunks)):
        fetch(k).start()

    def step(k, carry):
        @pl.when(k + DEPTH < chunks)
        def _():
            fetch(k + DEPTH).start()

        fetch(k).wait()
        for j in range(size):
            image = k * size + j
            total = jnp.zeros((8, patches), F32)
            square = jnp.zeros((8, patches), F32)
            for r in range(0, feats, STRIP):
                t = t_buf[image, r : r + STRIP, :].astype(F32)
                for q in range(0, STRIP, 8):
                    u = t[q : q + 8]
                    total += u
                    square += u * u
            s_ref[0, pl.ds(image, 1), :] = jnp.sum(total, axis=0, keepdims=True)
            s_ref[1, pl.ds(image, 1), :] = jnp.sum(square, axis=0, keepdims=True)
        return carry

    lax.fori_loop(0, chunks, step, 0)


def patch_stats(targets):
    images, feats, patches = targets.shape
    chunks = divisor(images, 16)
    return pl.pallas_call(
        stats_kernel,
        in_specs=[pl.BlockSpec(memory_space=pltpu.HBM)],
        out_specs=[pl.BlockSpec(memory_space=pltpu.VMEM)] * 2,
        out_shape=[
            jax.ShapeDtypeStruct((2, images, patches), F32),
            pltpu.VMEM(targets.shape, targets.dtype),
        ],
        scratch_shapes=[
            pltpu.SemaphoreType.DMA((chunks,)),
        ],
        cost_estimate=pl.CostEstimate(
            flops=5_000_000_000, bytes_accessed=targets.size * 2, transcendentals=0
        ),
        compiler_params=pltpu.CompilerParams(vmem_limit_bytes=20 * MIB),
        name="patch_stats",
    )(in_hbm(targets))


def stage_kernel(x_hbm, m_ref, x_ref, cov_ref, sem):
    copy = pltpu.make_async_copy(x_hbm.at[: x_ref.shape[0]], x_ref, sem)
    copy.start()
    for image in range(m_ref.shape[0]):
        cov_ref[image : image + 1, :] = jnp.sum(m_ref[image], axis=0, keepdims=True).astype(F32)
    copy.wait()


def stage_inputs(inputs, masks, images):
    shape = (images,) + inputs.shape[1:]
    return pl.pallas_call(
        stage_kernel,
        in_specs=[pl.BlockSpec(memory_space=pltpu.HBM), pl.BlockSpec(memory_space=pltpu.VMEM)],
        out_specs=[pl.BlockSpec(memory_space=pltpu.VMEM)] * 2,
        out_shape=[
            pltpu.VMEM(shape, inputs.dtype),
            jax.ShapeDtypeStruct((masks.shape[0], masks.shape[2]), F32),
        ],
        scratch_shapes=[pltpu.SemaphoreType.DMA],
        compiler_params=pltpu.CompilerParams(vmem_limit_bytes=20 * MIB),
        cost_estimate=pl.CostEstimate(
            flops=2_000_000_000, bytes_accessed=2 * inputs.size, transcendentals=0
        ),
        name="stage_inputs",
    )(in_hbm(inputs), masks)


def loss_kernel(
    feats_full, dp_axis,
    s1_ref, s2_ref, cov_ref, w_ref, b_ref, t_ref, head_ref, x_hbm,
    keep_a, send_a, keep_b, send_b,
    tail_ref, wt, bcol, rstd_s, shift_s, p0, p1, clip_s, acc, bacc, lacc, x_sem,
):
    images, feats, patches = t_ref.shape
    width = tail_ref.shape[2]
    head = head_ref.shape[0]
    steps = x_sem.shape[0]
    size = (images - head) // steps
    pred_s = p0, p1
    group = clip_s.shape[1] // patches

    def fetch(k):
        return pltpu.make_async_copy(
            x_hbm.at[pl.ds(head + k * size, size)], tail_ref.at[pl.ds(k * size, size)], x_sem.at[k]
        )

    for k in range(steps):
        fetch(k).start()

    wt[...] = w_ref[...].T
    bcol[...] = jnp.broadcast_to(b_ref[...].reshape(1, feats), (LANES, feats)).T
    acc[...] = jnp.zeros_like(acc)
    bacc[...] = jnp.zeros_like(bacc)
    lacc[...] = jnp.zeros_like(lacc)
    mean = (s1_ref[0] + s2_ref[0]) * (1.0 / feats_full)
    var = (s1_ref[1] + s2_ref[1]) * (1.0 / feats_full) - mean * mean
    rstd = lax.rsqrt(var + 1e-05)
    rstd_s[...] = rstd
    shift_s[...] = mean * rstd

    def predict(slot, x):
        pred_s[slot][...] = lax.dot_general(
            wt[...], x, (((1,), (1,)), ((), ())), preferred_element_type=F32
        )

    def elementwise(slot, image, at):
        row = pl.ds(image, 1)
        rstd_row, shift_row, cover = rstd_s[row, :], shift_s[row, :], cov_ref[row, :]
        losses = jnp.zeros((8, patches), F32)
        for r in range(0, feats, STRIP):
            t = t_ref[image, r : r + STRIP, :].astype(F32)
            bias = jnp.concatenate([bcol[r : r + STRIP, :]] * (patches // LANES), axis=1)
            d = (pred_s[slot][r : r + STRIP, :] + bias) + (shift_row - t * rstd_row)
            c = jnp.minimum(jnp.maximum(d, -1.0), 1.0)
            h = c * (d - 0.5 * c)
            for q in range(0, STRIP, 8):
                losses += h[q : q + 8]
            clipped = c * cover
            clip_s[r : r + STRIP, at * patches : (at + 1) * patches] = clipped.astype(BF16)
            folded = clipped[:, :LANES]
            for q in range(LANES, patches, LANES):
                folded += clipped[:, q : q + LANES]
            bacc[r : r + STRIP, :] += folded
        lacc[...] += losses * cover

    def run(x_ref, first, base, count):
        predict(0, x_ref[base])
        for g in range(count):
            if g + 1 < count:
                predict((g + 1) % 2, x_ref[base + g + 1])
            elementwise(g % 2, first + base + g, g % group)
            if (g + 1) % group == 0:
                rows = x_ref[pl.ds(base + g + 1 - group, group)].reshape(group * patches, width)
                acc[...] += jnp.dot(clip_s[...], rows, preferred_element_type=F32)

    def head_step(k, carry):
        run(head_ref, 0, k * size, size)
        return carry

    def tail_step(k, carry):
        fetch(k).wait()
        run(tail_ref, head, k * size, size)
        return carry

    lax.fori_loop(0, head // size, head_step, 0)
    lax.fori_loop(0, steps, tail_step, 0)

    grads = acc[...].T
    bias_row = jnp.sum(bacc[...].T, axis=0, keepdims=True)
    loss = jnp.sum(lacc[...])
    count = jnp.sum(cov_ref[...])
    lane = lax.broadcasted_iota(jnp.int32, (1, LANES), 1)
    scalars = jnp.where(lane == 0, loss, jnp.where(lane == 1, count, 0.0))
    parts = lax.axis_size(dp_axis)
    rows = width // parts
    me = lax.axis_index(dp_axis)
    cut, block = cut_rows(rows, feats), packed_rows(rows, feats)
    kept = (parts // 2) * cut
    for ref in (keep_a, send_a):
        ref[kept:, :] = jnp.zeros((EXTRA, LANES), F32)
        for k in range(-(-feats // LANES)):
            wide = min(LANES, feats - k * LANES)
            ref[kept + k : kept + k + 1, :wide] = bias_row[:, k * LANES : k * LANES + wide]
        ref[kept + EXTRA - 1 :, :] = scalars

    def put(ref, at, c, first, last):
        for lo, hi, where, (here, end, there) in pieces(rows, feats):
            low, high = max(where, first), min(where + hi - lo, last)
            if low < high:
                row = c * rows + lo + low - where
                ref[at + low - first : at + high - first, there : there + end - here] = grads[
                    row : row + high - low, here:end
                ]

    for bit in range(2):
        @pl.when(lax.rem(me, 2) == bit)
        def _():
            for c in range(parts):
                put(keep_a if c % 2 == bit else send_a, (c // 2) * cut, c, 0, cut)

        @pl.when(lax.rem(lax.div(me, 2), 2) == bit)
        def _():
            for c in range(parts):
                at = (c // 4 * 2 + c % 2) * (block - cut)
                put(keep_b if c // 2 % 2 == bit else send_b, at, c, cut, block)


def loss_and_grads(s1, s2, cover, weight, bias, targets, head, inputs, feats_full, dp_axis):
    images, feats, patches = targets.shape
    width = inputs.shape[2]
    rest = images - head.shape[0]
    size = divisor(math.gcd(rest, head.shape[0]), 32)
    group = divisor(size, 2)
    parts = lax.axis_size(dp_axis)
    cut, block = cut_rows(width // parts, feats), packed_rows(width // parts, feats)
    out_a = jax.ShapeDtypeStruct(((parts // 2) * cut + EXTRA, LANES), F32)
    out_b = jax.ShapeDtypeStruct(((parts // 2) * (block - cut), LANES), F32)
    return pl.pallas_call(
        functools.partial(loss_kernel, feats_full, dp_axis),
        in_specs=[pl.BlockSpec(memory_space=pltpu.VMEM)] * 7 + [pl.BlockSpec(memory_space=pltpu.HBM)],
        out_specs=[pl.BlockSpec(memory_space=pltpu.VMEM)] * 4,
        out_shape=[out_a, out_a, out_b, out_b],
        scratch_shapes=[
            pltpu.VMEM((rest,) + inputs.shape[1:], inputs.dtype),
            pltpu.VMEM((feats, width), BF16),
            pltpu.VMEM((feats, LANES), F32),
            pltpu.VMEM((images, patches), F32),
            pltpu.VMEM((images, patches), F32),
            pltpu.VMEM((feats, patches), F32),
            pltpu.VMEM((feats, patches), F32),
            pltpu.VMEM((feats, group * patches), BF16),
            pltpu.VMEM((feats, width), F32),
            pltpu.VMEM((feats, LANES), F32),
            pltpu.VMEM((8, patches), F32),
            pltpu.SemaphoreType.DMA((rest // size,)),
        ],
        compiler_params=pltpu.CompilerParams(vmem_limit_bytes=36 * MIB),
        cost_estimate=pl.CostEstimate(
            flops=images * patches * feats * width * 4,
            bytes_accessed=(targets.size + inputs.size) * 2,
            transcendentals=0,
        ),
        name="loss_and_grads",
    )(s1, s2, cover, weight, bias, in_vmem(targets), in_vmem(head), in_hbm(inputs))


def square_kernel(dp_axis, keep_ref, recv_ref, g_ref, tail_ref, out_ref):
    rows, feats = g_ref.shape
    block = packed_rows(rows, feats)
    both = keep_ref[...] + recv_ref[...]
    for lo, hi, where, lanes in pieces(rows, feats):
        g_ref[lo:hi, lanes[0] : lanes[1]] = both[
            where : where + hi - lo, lanes[2] : lanes[2] + lanes[1] - lanes[0]
        ]
    tail_ref[...] = both[block:]
    first = lax.axis_index(dp_axis) == 0
    grads = g_ref[...]
    bias = both[block : block + EXTRA - 1]
    loss = both[block + EXTRA - 1 :, 0:1]
    square = jnp.sum(grads * grads) + jnp.where(first, jnp.sum(bias * bias), 0.0)
    lane = lax.broadcasted_iota(jnp.int32, (1, LANES), 1)
    row = jnp.where(lane == 0, square, jnp.where((lane == 1) & first, loss, 0.0))
    out_ref[...] = jnp.broadcast_to(row, out_ref.shape)


def finish_kernel(feats_full, g_ref, tail_ref, all_ref, loss_ref, clip_ref, gw_ref, gb_ref):
    sums = jnp.sum(all_ref[...], axis=0, keepdims=True)
    square, loss = sums[:, 0:1], sums[:, 1:2]
    total = tail_ref[EXTRA - 1 :, 1:2]
    norm = jnp.sqrt(square) / total
    clip = jnp.minimum(1.0, 1.0 / (norm + 1e-06))
    factor = clip / total
    loss_ref[...] = loss / total / feats_full
    clip_ref[...] = clip
    gw_ref[...] = g_ref[...] * factor
    feats = gb_ref.shape[0]
    bias = tail_ref[...] * factor
    row = jnp.concatenate([bias[k : k + 1] for k in range(-(-feats // LANES))], axis=1)
    gb_ref[...] = row[:, :feats].reshape(feats)


def pairs(size, bit):
    return [(i, i ^ bit) for i in range(size)]


def swap(value, axis, bit):
    return lax.ppermute(value, axis, pairs(lax.axis_size(axis), bit))


def bits_of(size):
    return [1 << b for b in range(size.bit_length() - 1)]


def gather_far(weight, axis):
    size = lax.axis_size(axis)
    return [weight] + [swap(weight, axis, far) for far in range(2, size, 2)]


def swap_near(parts, lows, axis):
    half = len(parts)
    for bit in bits_of(half):
        low = lows[2 * bit]
        parts = [jnp.where(low, parts[j], parts[j ^ bit]) for j in range(half)]
    far = jnp.stack(parts)
    return far, swap(far, axis, 1)


def join_near(far, near, lows):
    half, rows, feats = far.shape
    low = lows[1]
    first, second = jnp.where(low, far, near), jnp.where(low, near, far)
    return jnp.stack([first, second], axis=1).reshape(2 * half * rows, feats)


def halve(value, block, low):
    pair = value.reshape(-1, 2, block, LANES)
    stay, go = jnp.where(low, pair[:, 0], pair[:, 1]), jnp.where(low, pair[:, 1], pair[:, 0])
    return stay.reshape(-1, LANES), go.reshape(-1, LANES)


def body(pred_input, proj_weight, proj_bias, targets, block_masks):
    feats = targets.shape[2]
    feats_full = float(feats * lax.axis_size("mp"))
    turned = jnp.swapaxes(targets, 1, 2)
    size = lax.axis_size("dp")
    me = lax.axis_index("dp")
    lows = {bit: (me & bit) == 0 for bit in bits_of(size)}
    lows, turned, proj_weight = lax.optimization_barrier((lows, turned, proj_weight))
    parts = gather_far(proj_weight, "dp")
    stats, turned = patch_stats(turned)
    parts, stats = lax.optimization_barrier((parts, stats))
    far, near = swap_near(parts, lows, "dp")
    mp_bits = bits_of(lax.axis_size("mp"))
    for bit in mp_bits[:-1]:
        stats = stats + swap(stats, "mp", bit)
    other = swap(stats, "mp", mp_bits[-1])
    staged, cover = stage_inputs(
        lax.optimization_barrier((pred_input, stats))[0], block_masks, targets.shape[0] // 2
    )
    near, staged = lax.optimization_barrier((near, staged))
    weight = join_near(far, near, lows)
    keep_a, send_a, keep_b, send_b = loss_and_grads(
        stats, other, cover, weight, proj_bias, turned, staged, pred_input, feats_full, "dp"
    )
    rows = pred_input.shape[2] // size
    cut, block = cut_rows(rows, feats), packed_rows(rows, feats)
    rest = block - cut
    parts = size // 2
    got_a, got_b = swap(send_a, "dp", 1), swap(send_b, "dp", 2)
    both_a = keep_a + got_a
    keep_a, send_a = halve(both_a[: parts * cut], cut, lows[2])
    extra = both_a[parts * cut :]
    got_a = swap(jnp.concatenate([send_a, extra], axis=0), "dp", 2)
    keep_b, send_b = halve(keep_b + got_b, rest, lows[1])
    got_b = swap(send_b, "dp", 1)
    parts //= 2
    both_a = jnp.concatenate([keep_a, extra], axis=0) + got_a
    extra = both_a[parts * cut :]
    main = jnp.concatenate(
        [both_a[: parts * cut].reshape(parts, cut, LANES), (keep_b + got_b).reshape(parts, rest, LANES)], axis=1
    ).reshape(parts * block, LANES)
    for bit in bits_of(size)[2:]:
        keep, send = halve(main, block, lows[bit])
        keep = jnp.concatenate([keep, extra], axis=0)
        received = swap(jnp.concatenate([send, extra], axis=0), "dp", bit)
        parts //= 2
        if parts > 1:
            both = keep + received
            main, extra = both[: parts * block], both[parts * block :]
    devices = size * lax.axis_size("mp")
    grads, tail, row = pl.pallas_call(
        functools.partial(square_kernel, "dp"),
        out_shape=[
            jax.ShapeDtypeStruct((rows, feats), F32),
            jax.ShapeDtypeStruct((EXTRA, LANES), F32),
            jax.ShapeDtypeStruct((devices, LANES), F32),
        ],
        compiler_params=pltpu.CompilerParams(vmem_limit_bytes=4 * MIB),
        name="square",
    )(keep, received)
    every = lax.all_to_all(row, ("dp", "mp"), 0, 0, tiled=True)
    loss, clip, grad_weight, grad_bias = pl.pallas_call(
        functools.partial(finish_kernel, feats_full),
        out_shape=[
            jax.ShapeDtypeStruct((1, 1), F32),
            jax.ShapeDtypeStruct((1, 1), F32),
            jax.ShapeDtypeStruct((rows, feats), F32),
            jax.ShapeDtypeStruct((feats,), F32),
        ],
        compiler_params=pltpu.CompilerParams(vmem_limit_bytes=4 * MIB),
        name="finish",
    )(grads, tail, every)
    return loss[0, 0], clip[0, 0], grad_weight, grad_bias


def solution(mesh):
    in_specs = (
        P("dp", None, None),
        P("dp", "mp"),
        P("mp"),
        P("dp", None, "mp"),
        P("dp", None, None),
    )
    out_specs = (P(), P(), P("dp", "mp"), P("mp"))
    return jax.shard_map(body, mesh=mesh, in_specs=in_specs, out_specs=out_specs, check_vma=False)
```

```python
import functools
import math

import jax
import jax.numpy as jnp
from jax import lax
from jax.experimental import pallas as pl
from jax.experimental.pallas import tpu as pltpu
from jax.sharding import PartitionSpec as P


F32, BF16 = jnp.float32, jnp.bfloat16
LANES = 128
STRIP = 16
EXTRA = 8
DEPTH = 8
MIB = 1 << 20


def divisor(count, most):
    return max(d for d in range(1, most + 1) if count % d == 0)


def in_hbm(value):
    return pltpu.with_memory_space_constraint(value, pltpu.HBM)


def in_vmem(value):
    return pltpu.with_memory_space_constraint(value, pltpu.VMEM)


def pieces(rows, feats):
    whole, left = divmod(feats, LANES)
    out = [(0, rows, k * rows, (k * LANES, (k + 1) * LANES, 0)) for k in range(whole)]
    if left:
        share = LANES // left if LANES % left == 0 and rows % (LANES // left) == 0 else 1
        each = rows // share
        for k in range(share):
            out.append((k * each, (k + 1) * each, whole * rows, (whole * LANES, feats, k * left)))
    return out


def packed_rows(rows, feats):
    return max(where + hi - lo for lo, hi, where, _ in pieces(rows, feats))


def cut_rows(rows, feats):
    return -(-packed_rows(rows, feats) // 16) * 8


def stats_kernel(t_hbm, s_ref, t_buf, t_sem):
    images, feats, patches = t_buf.shape
    chunks = t_sem.shape[0]
    size = images // chunks

    def fetch(k):
        rows = pl.ds(k * size, size)
        return pltpu.make_async_copy(t_hbm.at[rows], t_buf.at[rows], t_sem.at[k])

    for k in range(min(DEPTH, chunks)):
        fetch(k).start()

    def step(k, carry):
        @pl.when(k + DEPTH < chunks)
        def _():
            fetch(k + DEPTH).start()

        fetch(k).wait()
        for j in range(size):
            image = k * size + j
            total = jnp.zeros((8, patches), F32)
            square = jnp.zeros((8, patches), F32)
            for r in range(0, feats, STRIP):
                t = t_buf[image, r : r + STRIP, :].astype(F32)
                for q in range(0, STRIP, 8):
                    u = t[q : q + 8]
                    total += u
                    square += u * u
            s_ref[0, pl.ds(image, 1), :] = jnp.sum(total, axis=0, keepdims=True)
            s_ref[1, pl.ds(image, 1), :] = jnp.sum(square, axis=0, keepdims=True)
        return carry

    lax.fori_loop(0, chunks, step, 0)


def patch_stats(targets):
    images, feats, patches = targets.shape
    chunks = divisor(images, 16)
    return pl.pallas_call(
        stats_kernel,
        in_specs=[pl.BlockSpec(memory_space=pltpu.HBM)],
        out_specs=[pl.BlockSpec(memory_space=pltpu.VMEM)] * 2,
        out_shape=[
            jax.ShapeDtypeStruct((2, images, patches), F32),
            pltpu.VMEM(targets.shape, targets.dtype),
        ],
        scratch_shapes=[
            pltpu.SemaphoreType.DMA((chunks,)),
        ],
        cost_estimate=pl.CostEstimate(
            flops=5_000_000_000, bytes_accessed=targets.size * 2, transcendentals=0
        ),
        compiler_params=pltpu.CompilerParams(vmem_limit_bytes=20 * MIB),
        name="patch_stats",
    )(in_hbm(targets))


def stage_kernel(x_hbm, m_ref, x_ref, cov_ref, sem):
    copy = pltpu.make_async_copy(x_hbm.at[: x_ref.shape[0]], x_ref, sem)
    copy.start()
    for image in range(m_ref.shape[0]):
        cov_ref[image : image + 1, :] = jnp.sum(m_ref[image], axis=0, keepdims=True).astype(F32)
    copy.wait()


def stage_inputs(inputs, masks, images):
    shape = (images,) + inputs.shape[1:]
    return pl.pallas_call(
        stage_kernel,
        in_specs=[pl.BlockSpec(memory_space=pltpu.HBM), pl.BlockSpec(memory_space=pltpu.VMEM)],
        out_specs=[pl.BlockSpec(memory_space=pltpu.VMEM)] * 2,
        out_shape=[
            pltpu.VMEM(shape, inputs.dtype),
            jax.ShapeDtypeStruct((masks.shape[0], masks.shape[2]), F32),
        ],
        scratch_shapes=[pltpu.SemaphoreType.DMA],
        compiler_params=pltpu.CompilerParams(vmem_limit_bytes=20 * MIB),
        cost_estimate=pl.CostEstimate(
            flops=2_000_000_000, bytes_accessed=2 * inputs.size, transcendentals=0
        ),
        name="stage_inputs",
    )(in_hbm(inputs), masks)


def loss_kernel(
    feats_full, dp_axis,
    s1_ref, s2_ref, cov_ref, w_ref, b_ref, t_ref, head_ref, x_hbm,
    keep_a, send_a, keep_b, send_b,
    tail_ref, wt, bcol, rstd_s, shift_s, p0, p1, clip_s, acc, bacc, lacc, x_sem,
):
    images, feats, patches = t_ref.shape
    width = tail_ref.shape[2]
    head = head_ref.shape[0]
    steps = x_sem.shape[0]
    size = (images - head) // steps
    pred_s = p0, p1
    group = clip_s.shape[1] // patches

    def fetch(k):
        return pltpu.make_async_copy(
            x_hbm.at[pl.ds(head + k * size, size)], tail_ref.at[pl.ds(k * size, size)], x_sem.at[k]
        )

    for k in range(steps):
        fetch(k).start()

    wt[...] = w_ref[...].T
    bcol[...] = jnp.broadcast_to(b_ref[...].reshape(1, feats), (LANES, feats)).T
    acc[...] = jnp.zeros_like(acc)
    bacc[...] = jnp.zeros_like(bacc)
    lacc[...] = jnp.zeros_like(lacc)
    mean = (s1_ref[0] + s2_ref[0]) / feats_full
    var = (s1_ref[1] + s2_ref[1]) / feats_full - mean * mean
    rstd = lax.rsqrt(jnp.maximum(var, 0.0) + 1e-05)
    rstd_s[...] = rstd
    shift_s[...] = mean * rstd

    def predict(slot, x):
        pred_s[slot][...] = lax.dot_general(
            wt[...], x, (((1,), (1,)), ((), ())), preferred_element_type=F32
        )

    def elementwise(slot, image, at):
        row = pl.ds(image, 1)
        rstd_row, shift_row, cover = rstd_s[row, :], shift_s[row, :], cov_ref[row, :]
        losses = jnp.zeros((8, patches), F32)
        for r in range(0, feats, STRIP):
            t = t_ref[image, r : r + STRIP, :].astype(F32)
            bias = jnp.concatenate([bcol[r : r + STRIP, :]] * (patches // LANES), axis=1)
            d = (pred_s[slot][r : r + STRIP, :] + bias) + (shift_row - t * rstd_row)
            c = jnp.minimum(jnp.maximum(d, -1.0), 1.0)
            h = c * (d - 0.5 * c)
            for q in range(0, STRIP, 8):
                losses += h[q : q + 8]
            clipped = c * cover
            clip_s[r : r + STRIP, at * patches : (at + 1) * patches] = clipped.astype(BF16)
            folded = clipped[:, :LANES]
            for q in range(LANES, patches, LANES):
                folded += clipped[:, q : q + LANES]
            bacc[r : r + STRIP, :] += folded
        lacc[...] += losses * cover

    def run(x_ref, first, base, count):
        predict(0, x_ref[base])
        for g in range(count):
            if g + 1 < count:
                predict((g + 1) % 2, x_ref[base + g + 1])
            elementwise(g % 2, first + base + g, g % group)
            if (g + 1) % group == 0:
                rows = x_ref[pl.ds(base + g + 1 - group, group)].reshape(group * patches, width)
                acc[...] += jnp.dot(clip_s[...], rows, preferred_element_type=F32)

    def head_step(k, carry):
        run(head_ref, 0, k * size, size)
        return carry

    def tail_step(k, carry):
        fetch(k).wait()
        run(tail_ref, head, k * size, size)
        return carry

    lax.fori_loop(0, head // size, head_step, 0)
    lax.fori_loop(0, steps, tail_step, 0)

    grads = acc[...].T
    bias_row = jnp.sum(bacc[...].T, axis=0, keepdims=True)
    loss = jnp.sum(lacc[...])
    count = jnp.sum(cov_ref[...])
    lane = lax.broadcasted_iota(jnp.int32, (1, LANES), 1)
    scalars = jnp.where(lane == 0, loss, jnp.where(lane == 1, count, 0.0))
    parts = lax.axis_size(dp_axis)
    rows = width // parts
    me = lax.axis_index(dp_axis)
    cut, block = cut_rows(rows, feats), packed_rows(rows, feats)
    kept = (parts // 2) * cut
    for ref in (keep_a, send_a):
        ref[kept:, :] = jnp.zeros((EXTRA, LANES), F32)
        for k in range(-(-feats // LANES)):
            wide = min(LANES, feats - k * LANES)
            ref[kept + k : kept + k + 1, :wide] = bias_row[:, k * LANES : k * LANES + wide]
        ref[kept + EXTRA - 1 :, :] = scalars

    def put(ref, at, c, first, last):
        for lo, hi, where, (here, end, there) in pieces(rows, feats):
            low, high = max(where, first), min(where + hi - lo, last)
            if low < high:
                row = c * rows + lo + low - where
                ref[at + low - first : at + high - first, there : there + end - here] = grads[
                    row : row + high - low, here:end
                ]

    for bit in range(2):
        @pl.when(lax.rem(me, 2) == bit)
        def _():
            for c in range(parts):
                put(keep_a if c % 2 == bit else send_a, (c // 2) * cut, c, 0, cut)

        @pl.when(lax.rem(lax.div(me, 2), 2) == bit)
        def _():
            for c in range(parts):
                at = (c // 4 * 2 + c % 2) * (block - cut)
                put(keep_b if c // 2 % 2 == bit else send_b, at, c, cut, block)


def loss_and_grads(s1, s2, cover, weight, bias, targets, head, inputs, feats_full, dp_axis):
    images, feats, patches = targets.shape
    width = inputs.shape[2]
    rest = images - head.shape[0]
    size = divisor(math.gcd(rest, head.shape[0]), 32)
    group = divisor(size, 2)
    parts = lax.axis_size(dp_axis)
    cut, block = cut_rows(width // parts, feats), packed_rows(width // parts, feats)
    out_a = jax.ShapeDtypeStruct(((parts // 2) * cut + EXTRA, LANES), F32)
    out_b = jax.ShapeDtypeStruct(((parts // 2) * (block - cut), LANES), F32)
    return pl.pallas_call(
        functools.partial(loss_kernel, feats_full, dp_axis),
        in_specs=[pl.BlockSpec(memory_space=pltpu.VMEM)] * 7 + [pl.BlockSpec(memory_space=pltpu.HBM)],
        out_specs=[pl.BlockSpec(memory_space=pltpu.VMEM)] * 4,
        out_shape=[out_a, out_a, out_b, out_b],
        scratch_shapes=[
            pltpu.VMEM((rest,) + inputs.shape[1:], inputs.dtype),
            pltpu.VMEM((feats, width), BF16),
            pltpu.VMEM((feats, LANES), F32),
            pltpu.VMEM((images, patches), F32),
            pltpu.VMEM((images, patches), F32),
            pltpu.VMEM((feats, patches), F32),
            pltpu.VMEM((feats, patches), F32),
            pltpu.VMEM((feats, group * patches), BF16),
            pltpu.VMEM((feats, width), F32),
            pltpu.VMEM((feats, LANES), F32),
            pltpu.VMEM((8, patches), F32),
            pltpu.SemaphoreType.DMA((rest // size,)),
        ],
        compiler_params=pltpu.CompilerParams(vmem_limit_bytes=36 * MIB),
        cost_estimate=pl.CostEstimate(
            flops=images * patches * feats * width * 4,
            bytes_accessed=(targets.size + inputs.size) * 2,
            transcendentals=0,
        ),
        name="loss_and_grads",
    )(s1, s2, cover, weight, bias, in_vmem(targets), in_vmem(head), in_hbm(inputs))


def square_kernel(dp_axis, keep_ref, recv_ref, g_ref, tail_ref, out_ref):
    rows, feats = g_ref.shape
    block = packed_rows(rows, feats)
    both = keep_ref[...] + recv_ref[...]
    for lo, hi, where, lanes in pieces(rows, feats):
        g_ref[lo:hi, lanes[0] : lanes[1]] = both[
            where : where + hi - lo, lanes[2] : lanes[2] + lanes[1] - lanes[0]
        ]
    tail_ref[...] = both[block:]
    first = lax.axis_index(dp_axis) == 0
    grads = g_ref[...]
    bias = both[block : block + EXTRA - 1]
    loss = both[block + EXTRA - 1 :, 0:1]
    square = jnp.sum(grads * grads) + jnp.where(first, jnp.sum(bias * bias), 0.0)
    lane = lax.broadcasted_iota(jnp.int32, (1, LANES), 1)
    row = jnp.where(lane == 0, square, jnp.where((lane == 1) & first, loss, 0.0))
    out_ref[...] = jnp.broadcast_to(row, out_ref.shape)


def finish_kernel(feats_full, g_ref, tail_ref, all_ref, loss_ref, clip_ref, gw_ref, gb_ref):
    sums = jnp.sum(all_ref[...], axis=0, keepdims=True)
    square, loss = sums[:, 0:1], sums[:, 1:2]
    total = tail_ref[EXTRA - 1 :, 1:2]
    norm = jnp.sqrt(square) / total
    clip = jnp.minimum(1.0, 1.0 / (norm + 1e-06))
    factor = clip / total
    loss_ref[...] = loss / total / feats_full
    clip_ref[...] = clip
    gw_ref[...] = g_ref[...] * factor
    feats = gb_ref.shape[0]
    bias = tail_ref[...] * factor
    row = jnp.concatenate([bias[k : k + 1] for k in range(-(-feats // LANES))], axis=1)
    gb_ref[...] = row[:, :feats].reshape(feats)


def pairs(size, bit):
    return [(i, i ^ bit) for i in range(size)]


def swap(value, axis, bit):
    return lax.ppermute(value, axis, pairs(lax.axis_size(axis), bit))


def bits_of(size):
    return [1 << b for b in range(size.bit_length() - 1)]


def gather_far(weight, axis):
    size = lax.axis_size(axis)
    return [weight] + [swap(weight, axis, far) for far in range(2, size, 2)]


def swap_near(parts, lows, axis):
    half = len(parts)
    for bit in bits_of(half):
        low = lows[2 * bit]
        parts = [jnp.where(low, parts[j], parts[j ^ bit]) for j in range(half)]
    far = jnp.stack(parts)
    return far, swap(far, axis, 1)


def join_near(far, near, lows):
    half, rows, feats = far.shape
    low = lows[1]
    first, second = jnp.where(low, far, near), jnp.where(low, near, far)
    return jnp.stack([first, second], axis=1).reshape(2 * half * rows, feats)


def halve(value, block, low):
    pair = value.reshape(-1, 2, block, LANES)
    stay, go = jnp.where(low, pair[:, 0], pair[:, 1]), jnp.where(low, pair[:, 1], pair[:, 0])
    return stay.reshape(-1, LANES), go.reshape(-1, LANES)


def body(pred_input, proj_weight, proj_bias, targets, block_masks):
    feats = targets.shape[2]
    feats_full = float(feats * lax.axis_size("mp"))
    turned = jnp.swapaxes(targets, 1, 2)
    size = lax.axis_size("dp")
    me = lax.axis_index("dp")
    lows = {bit: (me & bit) == 0 for bit in bits_of(size)}
    lows, turned, proj_weight = lax.optimization_barrier((lows, turned, proj_weight))
    parts = gather_far(proj_weight, "dp")
    stats, turned = patch_stats(turned)
    parts, stats = lax.optimization_barrier((parts, stats))
    far, near = swap_near(parts, lows, "dp")
    mp_bits = bits_of(lax.axis_size("mp"))
    for bit in mp_bits[:-1]:
        stats = stats + swap(stats, "mp", bit)
    other = swap(stats, "mp", mp_bits[-1])
    staged, cover = stage_inputs(
        lax.optimization_barrier((pred_input, stats))[0], block_masks, targets.shape[0] // 2
    )
    near, staged = lax.optimization_barrier((near, staged))
    weight = join_near(far, near, lows)
    keep_a, send_a, keep_b, send_b = loss_and_grads(
        stats, other, cover, weight, proj_bias, turned, staged, pred_input, feats_full, "dp"
    )
    rows = pred_input.shape[2] // size
    cut, block = cut_rows(rows, feats), packed_rows(rows, feats)
    rest = block - cut
    parts = size // 2
    got_a, got_b = swap(send_a, "dp", 1), swap(send_b, "dp", 2)
    both_a = keep_a + got_a
    keep_a, send_a = halve(both_a[: parts * cut], cut, lows[2])
    extra = both_a[parts * cut :]
    got_a = swap(jnp.concatenate([send_a, extra], axis=0), "dp", 2)
    keep_b, send_b = halve(keep_b + got_b, rest, lows[1])
    got_b = swap(send_b, "dp", 1)
    parts //= 2
    both_a = jnp.concatenate([keep_a, extra], axis=0) + got_a
    extra = both_a[parts * cut :]
    main = jnp.concatenate(
        [both_a[: parts * cut].reshape(parts, cut, LANES), (keep_b + got_b).reshape(parts, rest, LANES)], axis=1
    ).reshape(parts * block, LANES)
    for bit in bits_of(size)[2:]:
        keep, send = halve(main, block, lows[bit])
        keep = jnp.concatenate([keep, extra], axis=0)
        received = swap(jnp.concatenate([send, extra], axis=0), "dp", bit)
        parts //= 2
        if parts > 1:
            both = keep + received
            main, extra = both[: parts * block], both[parts * block :]
    devices = size * lax.axis_size("mp")
    grads, tail, row = pl.pallas_call(
        functools.partial(square_kernel, "dp"),
        out_shape=[
            jax.ShapeDtypeStruct((rows, feats), F32),
            jax.ShapeDtypeStruct((EXTRA, LANES), F32),
            jax.ShapeDtypeStruct((devices, LANES), F32),
        ],
        compiler_params=pltpu.CompilerParams(vmem_limit_bytes=4 * MIB),
        name="square",
    )(keep, received)
    every = lax.all_to_all(row, ("dp", "mp"), 0, 0, tiled=True)
    loss, clip, grad_weight, grad_bias = pl.pallas_call(
        functools.partial(finish_kernel, feats_full),
        out_shape=[
            jax.ShapeDtypeStruct((1, 1), F32),
            jax.ShapeDtypeStruct((1, 1), F32),
            jax.ShapeDtypeStruct((rows, feats), F32),
            jax.ShapeDtypeStruct((feats,), F32),
        ],
        compiler_params=pltpu.CompilerParams(vmem_limit_bytes=4 * MIB),
        name="finish",
    )(grads, tail, every)
    return loss[0, 0], clip[0, 0], grad_weight, grad_bias


def solution(mesh):
    in_specs = (
        P("dp", None, None),
        P("dp", "mp"),
        P("mp"),
        P("dp", None, "mp"),
        P("dp", None, None),
    )
    out_specs = (P(), P(), P("dp", "mp"), P("mp"))
    return jax.shard_map(body, mesh=mesh, in_specs=in_specs, out_specs=out_specs, check_vma=False)
```
